32 devices in a mesh: field: 2 (over x), ep: 16 (over z, y, core).
Axes of the slice: x: 2, y: 2, z: 4, core: 2. Of those that a mesh axis runs over, the one named last changes fastest.
Arguments:
- images: float32 [64, 16, 256], P(('field', 'ep')), parts along dimension 0, may hold values from -6 to 6
- reference_image: float32 [32, 256], P('field'), parts along dimension 0, may hold values from -6 to 6
- kernels: float32 [16, 23, 23], replicated, may hold values from -0.25 to 0.25
- kernel_index: int32 [64], P(('field', 'ep')), parts along dimension 0, may hold values from 0 to 15
- tile_mask: int32 [64, 16, 2], P(('field', 'ep')), parts along dimension 0, may hold values 0 or 1
- systematics: float32 [64, 40], P('field'), parts along dimension 0, may hold values from -6 to 6
- onsets: int32 [16], P('field'), parts along dimension 0, may hold values from 0 to 27
Outputs:
- coefficients: float32 [48, 32, 256], P(None, ('field', 'ep')), parts along dimension 1
- epoch_scatter: float32 [64], P('field'), parts along dimension 0
The draws below stay inside these ranges and needn't reach their ends.
There are 2 independent parts, one for each index of `field`. The reference program is written for one: setup_inputs(seed, part) draws one part's arguments, and reference() takes and returns one part's arrays. A program takes and returns all parts, laid end to end along the dimension named above; an argument that names none is the same for every part. Nothing has to cross between parts.
All inputs are finite; a program needn't handle non-finite values. No bound on the sum of `tile_mask` on one device may be relied on, other than what follows from the above.
Results may differ from the reference program's by a relative error of at most 0.00011.
Values sent between devices are 32-bit elements; how exact they have to be, the bound alone decides.
No kernel may reach another device: no remote copies, remote signals or barrier semaphores. Data moves between devices by JAX's collectives and lax.ppermute only.
A program may use at most 64 MiB of HBM per device.

```python
import jax
import jax.numpy as jnp
from jax import lax

W = 256
KS = 23
NK = 16
NSYS = 40
NTR = 8
R = 16
E = 32


def touch_ends(drawn, stream_key, smallest, high):
    dims = drawn.shape
    spot = [jax.random.randint(jax.random.fold_in(stream_key, axis), (), 0, dims[axis]) for axis in range(len(dims))]
    drawn = drawn.at[tuple(spot)].set(smallest)
    longest = dims.index(max(dims))
    spot[longest] = (spot[longest] + 1) % dims[longest]
    return drawn.at[tuple(spot)].set(high)


def block_levels(rng, dims, cuts, least, largest):
    level, own = 1.0, jax.random.fold_in(rng, 6)
    for position, shards_of in cuts:
        steps = jnp.exp(jax.random.uniform(jax.random.fold_in(own, position), (shards_of,), jnp.float32, least / len(cuts), largest / len(cuts)))
        level = level * jnp.repeat(steps, dims[position] // shards_of).reshape([-1 if axis == position else 1 for axis in range(len(dims))])
    return level


def noise(stream_key, dims, scale, reach, shards=(), kind=jnp.bfloat16):
    factor_of = block_levels(stream_key, dims, shards, -0.22, 0.18) if shards else 1.0
    values = jax.random.normal(stream_key, dims, jnp.float32) * scale * factor_of
    return jnp.minimum(jnp.maximum(values, -reach), reach).astype(kind)


def setup_inputs(seed: int = 0, part: int = 0) -> dict:
    splits = jax.random.split(jax.random.key(seed), 8)
    own_keys = jax.random.split(jax.random.fold_in(splits[7], part), 8)
    images = noise(own_keys[0], (E, R, W), 1.0, 6.0, ((0, 16),), jnp.float32)
    reference_image = noise(own_keys[1], (R, W), 1.0, 6.0, (), jnp.float32)
    kernels = noise(splits[2], (NK, KS, KS), (KS * KS) ** -0.5, 0.25, (), jnp.float32)
    kernel_index = touch_ends(jax.random.randint(own_keys[3], (E,), 0, NK), jax.random.fold_in(own_keys[3], 1), 0, NK - 1).astype(jnp.int32)
    tile_mask = touch_ends((jax.random.randint(own_keys[4], (E, R, W // 128), 0, 8) < 7).astype(jnp.int32), jax.random.fold_in(own_keys[4], 1), 0, 1)
    systematics = noise(own_keys[5], (E, NSYS), 1.0, 6.0, (), jnp.float32)
    onsets = touch_ends(jax.random.randint(own_keys[6], (NTR,), 0, E - 4), jax.random.fold_in(own_keys[6], 1), 0, (E - 4) - 1).astype(jnp.int32)
    return dict(images=images, reference_image=reference_image, kernels=kernels, kernel_index=kernel_index, tile_mask=tile_mask, systematics=systematics, onsets=onsets)


cov_ridge = 0.5
fit_ridge = 1.0

def correlate(stack, chosen):
    count = stack.shape[0]
    filters = jnp.transpose(chosen, (1, 2, 0))[:, :, None, :]
    result = lax.conv_general_dilated(stack[None], filters, (1, 1), 'SAME', dimension_numbers=('NCHW', 'HWIO', 'NCHW'), feature_group_count=count, precision=lax.Precision.HIGHEST)
    return result[0]

def subtract(stack, reference_image, chosen, masks):
    result = reference_image[None] - correlate(stack, chosen)
    shape = result.shape
    tiles = result.reshape(shape[0], shape[1], shape[2] // 128, 128) * masks[..., None].astype(jnp.float32)
    return tiles.reshape(shape)

def build_design(systematics, onsets):
    count = systematics.shape[0]
    templates = onsets.shape[0]
    epoch_axis = jnp.arange(count, dtype=jnp.float32)[:, None]
    delays = epoch_axis - onsets[None, :].astype(jnp.float32)
    timescale = (jnp.arange(templates, dtype=jnp.float32) + 1.0) * count / (2.0 * templates)
    transient = jnp.where(delays >= 0.0, jnp.exp(-jnp.maximum(delays, 0.0) / timescale[None, :]), 0.0)
    return jnp.concatenate([systematics, transient.astype(systematics.dtype)], axis=1)

def fit_matrix(scatter, npixels, design):
    count = design.shape[0]
    columns = design.shape[1]
    covariance = scatter / npixels + cov_ridge * jnp.eye(count, dtype=scatter.dtype)
    lower = jnp.linalg.cholesky(covariance)
    weighted = jax.scipy.linalg.cho_solve((lower, True), design)
    normal = jnp.dot(design.T, weighted, precision=lax.Precision.HIGHEST) + fit_ridge * jnp.eye(columns, dtype=scatter.dtype)
    lower_fit = jnp.linalg.cholesky(normal)
    return jax.scipy.linalg.cho_solve((lower_fit, True), weighted.T)

def reference(images, reference_image, kernels, kernel_index, tile_mask, systematics, onsets):
    count, rows, width = images.shape
    chosen = kernels[kernel_index]
    difference = subtract(images, reference_image, chosen, tile_mask)
    pixel_data = difference.reshape(count, rows * width)
    scatter = jnp.dot(pixel_data, pixel_data.T, precision=lax.Precision.HIGHEST)
    npixels = float(rows * width)
    design = build_design(systematics, onsets)
    fit = fit_matrix(scatter, npixels, design)
    coefficients = jnp.dot(fit, pixel_data, precision=lax.Precision.HIGHEST)
    residual = pixel_data - jnp.dot(design, coefficients, precision=lax.Precision.HIGHEST)
    epoch_scatter = jnp.sum(residual * residual, axis=1) / npixels
    return (coefficients.reshape(design.shape[1], rows, width), epoch_scatter)
```

```python
import functools

import jax
import jax.numpy as jnp
from jax import lax
from jax.experimental import pallas as pl
from jax.experimental.pallas import tpu as pltpu
from jax.sharding import PartitionSpec as P

cov_ridge = 0.5
LANES = 128
HI = lax.Precision.HIGHEST


def split(x):
    top = x.astype(jnp.bfloat16)
    return top, (x - top.astype(jnp.float32)).astype(jnp.bfloat16)


def mm(a, b, dims):
    return lax.dot_general(a, b, (dims, ((), ())), preferred_element_type=jnp.float32)


def mm3(a, b, dims):
    a1, a2 = split(a)
    b1, b2 = split(b)
    return mm(a1, b1, dims) + (mm(a1, b2, dims) + mm(a2, b1, dims))


def mmh(a, b, dims):
    return lax.dot_general(
        a, b, (dims, ((), ())), precision=HI, preferred_element_type=jnp.float32
    )


NN = ((1,), (0,))
NT = ((1,), (1,))
TN = ((0,), (0,))


def subtract_kernel(index, images, reference_image, table, masks, out, padded, taps):
    count, rows, width = images.shape
    side = table.shape[0]
    half = (side - 1) // 2
    wide = padded.shape[1]
    per_tile = LANES // rows
    tiles = -(-side // per_tile)
    lane = lax.broadcasted_iota(jnp.int32, (rows, LANES), 1)
    tile_of = lax.broadcasted_iota(jnp.int32, (masks.shape[1], width), 1) // 128
    tile_row = lax.broadcasted_iota(jnp.int32, (masks.shape[1], width), 0)
    spread = (tile_of == tile_row).astype(jnp.float32)
    padded[:, width:] = jnp.zeros((rows, wide - width), jnp.float32)
    for e in range(count):
        chosen = index[e]
        taps[...] = jnp.zeros(taps.shape, jnp.float32)
        for a in range(side):
            taps[a : a + 1, :side] = table[a, pl.ds(chosen, 1), :]
        flipped = pltpu.roll(jnp.transpose(taps[...])[: -(-side // 8) * 8], LANES - half, 1)
        blocks = []
        for t in range(tiles):
            block = jnp.zeros((rows, LANES), jnp.float32)
            for j in range(per_tile):
                b = t * per_tile + j
                if b >= side:
                    continue
                column = jnp.broadcast_to(flipped[b : b + 1, :], (rows, LANES))
                moved = pltpu.roll(
                    column, j * rows, 1, stride=1, stride_axis=0
                )
                here = (lane >= j * rows) & (lane < (j + 1) * rows)
                block = jnp.where(here, moved, block)
            blocks.append(block)
        toeplitz = jnp.concatenate(blocks, axis=1) if tiles > 1 else blocks[0]
        padded[:, :width] = images[e]
        image = padded[...]
        shifted = [
            (pltpu.roll(image, (half - b) % wide, 1) if b != half else image)[:, :width]
            for b in range(side)
        ]
        extra = tiles * per_tile - side
        if extra:
            shifted.append(jnp.zeros((extra * rows, width), jnp.float32))
        stacked = jnp.concatenate(shifted, axis=0)
        model = mm3(toeplitz, stacked, NN)
        good = mm(masks[e].astype(jnp.float32), spread, TN)
        result = (reference_image[...] - model) * good
        for t in range(width // LANES):
            out[e, t] = result[:, t * LANES : (t + 1) * LANES]


def fit_kernel(
    place, near, far, systematics, onsets, coefficients, epoch_scatter, *, rows, order
):
    total = near.shape[0] + far.shape[0]
    count = systematics.shape[0]
    stride = total // count
    width = stride // rows * LANES
    templates = onsets.shape[1]
    npixels = float(rows * width)
    local_bits = (count >> len(order)).bit_length() - 1

    def at(r):
        return jnp.concatenate(
            [half[pl.ds(r, count // 2, stride=stride), :] for half in (near, far)], axis=0
        )

    def true_epoch(here):
        block = here >> local_bits
        flip = jnp.zeros_like(here)
        for b, bit in enumerate(order):
            flip = flip | (((block >> b) & 1) << bit)
        return ((flip ^ place[0]) << local_bits) | (here & ((1 << local_bits) - 1))

    pieces = [at(r) for r in range(stride)]
    pixels = jnp.concatenate(pieces, axis=1)
    top, low = split(pixels)
    first = mm(top, top, NT)
    cross = mm(top, low, NT)
    scatter = first + (cross + jnp.transpose(cross))
    at_row = lax.broadcasted_iota(jnp.int32, (count, count), 0)
    at_col = lax.broadcasted_iota(jnp.int32, (count, count), 1)
    eye = (at_row == at_col).astype(jnp.float32)
    covariance = scatter / npixels + cov_ridge * eye
    epoch = true_epoch(lax.broadcasted_iota(jnp.int32, (count, templates), 0))
    moved = true_epoch(at_row) == at_col
    delays = (epoch - onsets[...]).astype(jnp.float32)
    which = lax.broadcasted_iota(jnp.int32, (count, templates), 1).astype(jnp.float32)
    timescale = (which + 1.0) * (count / (2.0 * templates))
    transient = jnp.where(delays >= 0.0, jnp.exp(-jnp.maximum(delays, 0.0) / timescale), 0.0)
    regressors = mmh(moved.astype(jnp.float32), systematics[...], NN)
    design = jnp.concatenate([regressors, transient], axis=1)
    whole = covariance + mmh(design, design, NT)
    work = jnp.concatenate([whole, eye], axis=1)
    wide_row = lax.broadcasted_iota(jnp.int32, (count, 1), 0)
    for k in range(count):
        column = work[:, k : k + 1]
        pivot = work[k : k + 1, :] / work[k : k + 1, k : k + 1]
        work = jnp.where(wide_row == k, pivot, work - column * pivot)
    inverse = work[:, count:]
    block_rows = rows >> len(order)
    fit = mmh(jnp.transpose(design), inverse, NN)
    for b in range(block_rows):
        line = place[0] * block_rows + b
        chunks = []
        for t in range(0, stride, rows):
            chunk = pieces[t]
            for r in range(1, rows):
                chunk = jnp.where(line == r, pieces[t + r], chunk)
            chunks.append(chunk)
        own = jnp.concatenate(chunks, axis=1)
        coefficients[:, b * width : (b + 1) * width] = mmh(fit, own, NN)
    projector = mmh(covariance, inverse, NN)
    product = mmh(projector, scatter, NN)
    per_epoch = jnp.sum(product * projector, axis=1, keepdims=True) * (1.0 / npixels)
    epoch_scatter[...] = jnp.sum(jnp.where(moved, per_epoch, 0.0), axis=0, keepdims=True)


def shards(images, reference_image, kernels, kernel_index, tile_mask, systematics, onsets):
    local_count, rows, width = images.shape
    side = kernels.shape[1]
    vmem = pl.BlockSpec(memory_space=pltpu.VMEM)
    smem = pl.BlockSpec(memory_space=pltpu.SMEM)
    difference = pl.pallas_call(
        subtract_kernel,
        out_shape=jax.ShapeDtypeStruct((local_count, width // LANES, rows, LANES), jnp.float32),
        in_specs=[smem, vmem, vmem, vmem, vmem],
        out_specs=vmem,
        scratch_shapes=[
            pltpu.VMEM((rows, width + LANES), jnp.float32),
            pltpu.VMEM((LANES, LANES), jnp.float32),
        ],
        name="subtract",
    )(
        kernel_index,
        images,
        reference_image,
        jnp.transpose(kernels, (1, 0, 2)),
        jnp.transpose(tile_mask, (0, 2, 1)),
    )
    count = systematics.shape[0]
    devices = lax.axis_size("ep")
    near, far = gather(difference.reshape(-1, LANES), devices)
    block_rows = rows // devices
    place = lax.axis_index("ep").astype(jnp.int32).reshape(1)
    columns = systematics.shape[1] + onsets.shape[0]
    coefficients, epoch_scatter = pl.pallas_call(
        functools.partial(fit_kernel, rows=rows, order=exchange_order(devices)),
        out_shape=(
            jax.ShapeDtypeStruct((columns, block_rows * width), jnp.float32),
            jax.ShapeDtypeStruct((1, count), jnp.float32),
        ),
        in_specs=[smem, vmem, vmem, vmem, vmem],
        out_specs=(vmem, vmem),
        name="fit",
    )(place, near, far, systematics, onsets.reshape(1, -1))
    return (coefficients.reshape(columns, block_rows, width), epoch_scatter.reshape(count))


def exchange_order(devices):
    bits = devices.bit_length() - 1
    if bits < 2:
        return list(range(bits))
    return [bits - 2, bits - 1] + list(range(bits - 3, -1, -1))


def swap(block, devices, flip):
    return lax.ppermute(block, "ep", [(i, i ^ flip) for i in range(devices)])


def gather(block, devices):
    order = exchange_order(devices)
    if len(order) > 2:
        low, high = 1 << order[0], 1 << order[1]
        parts = [block] + [swap(block, devices, flip) for flip in (low, high, low | high)]
        block = jnp.concatenate(parts, axis=0)
        order = order[2:]
    for bit in order[:-1]:
        block = jnp.concatenate([block, swap(block, devices, 1 << bit)], axis=0)
    return block, swap(block, devices, 1 << order[-1])


def solution(mesh):
    in_specs = (
        P(("field", "ep"), None, None),
        P("field", None),
        P(),
        P(("field", "ep")),
        P(("field", "ep"), None, None),
        P("field", None),
        P("field"),
    )
    out_specs = (P(None, ("field", "ep"), None), P("field"))
    return jax.shard_map(shards, mesh=mesh, in_specs=in_specs, out_specs=out_specs, check_vma=False)
```
